32 devices in a mesh: grid: 8 (over z, x), band: 4 (over y, core).
Axes of the slice: x: 2, y: 2, z: 4, core: 2. Of those that a mesh axis runs over, the one named last changes fastest.
Arguments:
- psi: bfloat16 [2048, 16, 512], P('band', 'grid'), may hold values from -6 to 6
- ritz_matrix: float32 [2048, 2048], P('band'), may hold values from -0.125 to 0.125
- potential: float32 [16, 512], P('grid'), may hold values from 0.5 to 10, as said below
Outputs:
- rotated: bfloat16 [2048, 16, 512], P('band', 'grid')
- search: bfloat16 [2048, 16, 512], P('band', 'grid')
The draws below stay inside these ranges and needn't reach their ends.
Inputs may be any that keep to these rules, and one draw needn't show every extreme that they name: `potential`: positive everywhere.
All inputs are finite; a program needn't handle non-finite values.
Results may differ from the reference program's by a relative error of at most 0.0049.
Values may be sent and summed in bfloat16 or wider, within the bound.
A program may use at most 64 MiB of HBM per device.

```python
import jax
import jax.numpy as jnp
from jax import lax

B = 2048
NY = 8
NZ = 64
NX = 16


def draw_potential(key, part):
    first_key = jax.random.fold_in(key, 11)
    rough = jnp.exp(jax.random.uniform(first_key, (NX, NY * NZ), jnp.float32, jnp.log(0.5), jnp.log(2.0)))
    ramp = 1.0 + 2.0 * jnp.arange(NX, dtype=jnp.float32)[:, None] / NX
    return rough * ramp


def steps_of(stream_key, shape, split, least, largest):
    loudness = 1.0
    for position, blocks in split:
        draws = jax.random.uniform(jax.random.fold_in(jax.random.fold_in(stream_key, 6), position), (blocks,), jnp.float32, least / len(split), largest / len(split))
        loudness = loudness * jnp.repeat(jnp.exp(draws), shape[position] // blocks).reshape((-1,) + (1,) * (len(shape) - 1 - position))
    return loudness


def gaussian(own_key, shape, spread, bound, cuts=(), kind=jnp.bfloat16):
    drawn = spread * jax.random.normal(own_key, shape, jnp.float32)
    if cuts:
        drawn = drawn * steps_of(own_key, shape, cuts, -0.22, 0.18)
    return jnp.clip(drawn, -bound, bound).astype(kind)


def setup_inputs(seed: int = 0) -> dict:
    splits = jax.random.split(jax.random.key(seed), 4)
    return {
        "psi": gaussian(splits[0], (B, NX, NY * NZ), 1.0, 6.0, ((0, 4), (1, 8))),
        "ritz_matrix": gaussian(splits[1], (B, B), B ** -0.5, 0.125, ((0, 4),), jnp.float32),
        "potential": draw_potential(jax.random.fold_in(splits[3], 71), 0),
    }


epsilon_mean = 1e-06

def reference(psi, ritz_matrix, potential):
    flattened = psi.reshape(B, -1).astype(jnp.float32)
    product = jnp.dot(ritz_matrix, flattened, precision=lax.Precision.HIGHEST)
    rotated = product.reshape(B, NX, NY * NZ).astype(jnp.bfloat16)
    center = rotated.astype(jnp.float32).reshape(B, NX, NY, NZ)
    laplacian = -6.0 * center
    for axis_number in (1, 2, 3):
        laplacian = laplacian + jnp.roll(center, 1, axis_number) + jnp.roll(center, -1, axis_number)
    field_pot = potential.reshape(1, NX, NY, NZ)
    resid = -0.5 * laplacian + field_pot * center
    total_cells = NX * NY * NZ
    m_cross = lax.optimization_barrier(jnp.sum(center * resid, axis=(1, 2, 3))) / total_cells
    m_self = lax.optimization_barrier(jnp.sum(center * center, axis=(1, 2, 3))) / total_cells + epsilon_mean
    ratio = m_cross / m_self
    direction = resid - ratio[:, None, None, None] * center
    m_dir = lax.optimization_barrier(jnp.sum(direction * direction, axis=(1, 2, 3))) / total_cells
    search = direction * lax.rsqrt(m_dir + epsilon_mean)[:, None, None, None]
    return (rotated, search.reshape(B, NX, NY * NZ).astype(jnp.bfloat16))
```

```python
import functools

import jax
import jax.numpy as jnp
from jax import lax
from jax.experimental import pallas as pl
from jax.experimental.pallas import tpu as pltpu
from jax.sharding import PartitionSpec as P

NZ = 64
CW = 128
EPS = 1e-06
MESH = pl.DeviceIdType.MESH


def fused(nb, ng, psi, ritz, pot, rot_out, search_out,
          ritz_f, ritz_s, buf, acc, stencil, rot, halo, resid, part, sums, gat,
          own_sem, ritz_sem, out_sem, far_send, far_recv, near_send, near_recv,
          fwd_send, fwd_recv, halo_send, halo_recv, red_send, red_recv):
    planes, bands, cells = rot.shape
    nq = cells // CW
    chunks = [(p, q) for q in range(nq) for p in range(planes)]
    nchip = nb // 2
    b = lax.axis_index("band")
    g = lax.axis_index("grid")
    chip, core = b // 2, b % 2
    sib = chip * 2 + (1 - core)
    up, down = lax.rem(g + 1, ng), lax.rem(g + ng - 1, ng)

    def far_of(o):
        return lax.rem(chip + o, nchip)

    barrier = pltpu.get_barrier_semaphore()
    for o in range(1, nchip):
        pl.semaphore_signal(barrier, inc=1, device_id={"band": far_of(o) * 2 + core}, device_id_type=MESH)
    pl.semaphore_signal(barrier, inc=1, device_id={"band": sib}, device_id_type=MESH)
    for o in range(1, ng):
        pl.semaphore_signal(barrier, inc=1, device_id={"grid": lax.rem(g + o, ng)}, device_id_type=MESH)

    ritz_copy = pltpu.make_async_copy(ritz, ritz_f, ritz_sem)
    own = []
    for c, (p, q) in enumerate(chunks):
        own.append(pltpu.make_async_copy(psi.at[p, :, pl.ds(q * CW, CW)], buf.at[c, b], own_sem.at[c]))
    for copy in own:
        copy.start()
    ritz_copy.start()

    pl.semaphore_wait(barrier, nchip - 1 + 1 + ng - 1)

    far = {}
    near = []
    for c, (p, q) in enumerate(chunks):
        for o in range(1, nchip):
            copy = pltpu.make_async_remote_copy(
                src_ref=psi.at[p, :, pl.ds(q * CW, CW)], dst_ref=buf.at[c, b],
                send_sem=far_send.at[c, o - 1], recv_sem=far_recv.at[c, o - 1],
                device_id={"band": far_of(o) * 2 + core}, device_id_type=MESH)
            copy.start()
            far[c, o] = copy
        copy = pltpu.make_async_remote_copy(
            src_ref=psi.at[p, :, pl.ds(q * CW, CW)], dst_ref=buf.at[c, b],
            send_sem=near_send.at[c], recv_sem=near_recv.at[c],
            device_id={"band": sib}, device_id_type=MESH)
        copy.start()
        near.append(copy)

    row = lax.broadcasted_iota(jnp.int32, (cells, cells), 0)
    col = lax.broadcasted_iota(jnp.int32, (cells, cells), 1)
    ny = cells // NZ

    def hits(dy, dz):
        y = lax.rem(col // NZ + dy + ny, ny)
        z = lax.rem(lax.rem(col, NZ) + dz + NZ, NZ)
        return (row == y * NZ + z).astype(jnp.float32)

    mat = -6.0 * (row == col).astype(jnp.float32)
    for dy, dz in ((1, 0), (-1, 0), (0, 1), (0, -1)):
        mat = mat + hits(dy, dz)
    stencil[...] = mat.astype(jnp.bfloat16)

    ritz_copy.wait()
    rows = min(bands, 32)

    def split(i, carry):
        at = pl.ds(pl.multiple_of(i * rows, rows), rows)
        whole = ritz_f[at, :]
        hi = whole.astype(jnp.bfloat16)
        rest = whole - hi.astype(jnp.float32)
        mid = rest.astype(jnp.bfloat16)
        ritz_s[0, at, :] = hi
        ritz_s[1, at, :] = mid
        ritz_s[2, at, :] = (rest - mid.astype(jnp.float32)).astype(jnp.bfloat16)
        return carry

    lax.fori_loop(0, bands // rows, split, 0)

    def product(block, first, width):
        at = pl.ds(pl.multiple_of(first * bands, width), width)
        total = jnp.dot(ritz_s[0, :, at], block, preferred_element_type=jnp.float32)
        total += jnp.dot(ritz_s[1, :, at], block, preferred_element_type=jnp.float32)
        total += jnp.dot(ritz_s[2, :, at], block, preferred_element_type=jnp.float32)
        return total

    pair = 2 * bands
    for c in range(len(chunks)):
        own[c].wait()
        near[c].wait_recv()
        acc[c] = product(buf[c, pl.ds(chip * 2, 2)].reshape(pair, CW), chip * 2, pair)

    halos = []
    for c, (p, q) in enumerate(chunks):
        forwards = []
        for o in range(1, nchip):
            src = far_of(nchip - o) * 2 + core
            far[c, o].wait_recv()
            copy = pltpu.make_async_remote_copy(
                src_ref=buf.at[c, src], dst_ref=buf.at[c, src],
                send_sem=fwd_send.at[c, o - 1], recv_sem=fwd_recv.at[c, o - 1],
                device_id={"band": sib}, device_id_type=MESH)
            copy.start()
            forwards.append(copy)
        for o in range(1, nchip):
            forwards[o - 1].wait_recv()
            there = far_of(nchip - o) * 2
            acc[c] += product(buf[c, pl.ds(there, 2)].reshape(pair, CW), there, pair)
        at = pl.ds(q * CW, CW)
        rot[p, :, at] = acc[c].astype(jnp.bfloat16)
        for side, edge, to in ((0, planes - 1, up), (1, 0, down)):
            if p == edge:
                copy = pltpu.make_async_remote_copy(
                    src_ref=rot.at[p, :, at], dst_ref=halo.at[side, q],
                    send_sem=halo_send.at[side, q], recv_sem=halo_recv.at[side, q],
                    device_id={"grid": to}, device_id_type=MESH)
                copy.start()
                halos.append((side, q, copy))
        for copy in forwards:
            copy.wait_send()

    rot_copy = pltpu.make_async_copy(rot, rot_out, out_sem)
    rot_copy.start()

    vr = min(bands, 64)
    for p in range(planes):
        def local(i, carry):
            at = pl.ds(pl.multiple_of(i * vr, vr), vr)
            center = rot[p, at, :]
            lap = jnp.dot(center, stencil[...], preferred_element_type=jnp.float32)
            for other in (p - 1, p + 1):
                if 0 <= other < planes:
                    lap += rot[other, at, :].astype(jnp.float32)
            resid[p, at, :] = -0.5 * lap + pot[pl.ds(p, 1), :] * center.astype(jnp.float32)
            return carry

        lax.fori_loop(0, bands // vr, local, 0)

    part[...] = jnp.zeros_like(part)

    def gather_sums(p, q):
        def body(i, carry):
            at = pl.ds(pl.multiple_of(i * vr, vr), vr)
            lanes = pl.ds(q * CW, CW)
            center = rot[p, at, lanes].astype(jnp.float32)
            value = resid[p, at, lanes]
            if p == 0:
                value -= 0.5 * halo[0, q, at, :].astype(jnp.float32)
            if p == planes - 1:
                value -= 0.5 * halo[1, q, at, :].astype(jnp.float32)
            resid[p, at, lanes] = value
            part[0, at, :] += center * value
            part[1, at, :] += center * center
            part[2, at, :] += value * value
            return carry

        lax.fori_loop(0, bands // vr, body, 0)

    for q in range(nq):
        for side, hq, copy in halos:
            if hq == q:
                copy.wait_recv()
        for p in range(planes):
            gather_sums(p, q)

    for k in range(3):
        sums[pl.ds(k, 1), :] = jnp.sum(part[k].T, axis=0, keepdims=True)
    sums[pl.ds(3, 1), :] = jnp.zeros((1, bands), jnp.float32)

    reds = []
    for o in range(1, ng):
        copy = pltpu.make_async_remote_copy(
            src_ref=sums, dst_ref=gat.at[o - 1],
            send_sem=red_send.at[o - 1], recv_sem=red_recv.at[o - 1],
            device_id={"grid": lax.rem(g + o, ng)}, device_id_type=MESH)
        copy.start()
        reds.append(copy)
    total = sums[...]
    for o in range(1, ng):
        reds[o - 1].wait_recv()
        total = total + gat[o - 1]

    count = float(planes * cells * ng)
    m_cross = total[0:1] / count
    m_plain = total[1:2] / count
    ratio = m_cross / (m_plain + EPS)
    m_dir = total[2:3] / count - 2.0 * ratio * m_cross + ratio * ratio * m_plain
    scale = lax.rsqrt(m_dir + EPS)
    part[0] = jnp.broadcast_to(ratio, (CW, bands)).T
    part[1] = jnp.broadcast_to(scale, (CW, bands)).T

    for p in range(planes):
        def last(i, carry):
            at = pl.ds(pl.multiple_of(i * vr, vr), vr)
            for q in range(nq):
                lanes = pl.ds(q * CW, CW)
                direction = resid[p, at, lanes] - part[0, at, :] * rot[p, at, lanes].astype(jnp.float32)
                search_out[p, at, lanes] = (direction * part[1, at, :]).astype(jnp.bfloat16)
            return carry

        lax.fori_loop(0, bands // vr, last, 0)

    rot_copy.wait()
    for copy in far.values():
        copy.wait_send()
    for copy in near:
        copy.wait_send()
    for _, _, copy in halos:
        copy.wait_send()
    for copy in reds:
        copy.wait_send()


def shards(nb, ng, psi, ritz_matrix, potential):
    bands, planes, cells = psi.shape
    total = ritz_matrix.shape[1]
    nq = cells // CW
    nch = nq * planes
    far = max(nb // 2 - 1, 1)
    dma = pltpu.SemaphoreType.DMA
    rot, search = pl.pallas_call(
        functools.partial(fused, nb, ng),
        out_shape=[jax.ShapeDtypeStruct((planes, bands, cells), jnp.bfloat16)] * 2,
        in_specs=[pl.BlockSpec(memory_space=pl.ANY), pl.BlockSpec(memory_space=pl.ANY),
                  pl.BlockSpec(memory_space=pltpu.VMEM)],
        out_specs=[pl.BlockSpec(memory_space=pl.ANY), pl.BlockSpec(memory_space=pltpu.VMEM)],
        scratch_shapes=[
            pltpu.VMEM((bands, total), jnp.float32),
            pltpu.VMEM((3, bands, total), jnp.bfloat16),
            pltpu.VMEM((nch, nb, bands, CW), jnp.bfloat16),
            pltpu.VMEM((nch, bands, CW), jnp.float32),
            pltpu.VMEM((cells, cells), jnp.bfloat16),
            pltpu.VMEM((planes, bands, cells), jnp.bfloat16),
            pltpu.VMEM((2, nq, bands, CW), jnp.bfloat16),
            pltpu.VMEM((planes, bands, cells), jnp.float32),
            pltpu.VMEM((3, bands, CW), jnp.float32),
            pltpu.VMEM((4, bands), jnp.float32),
            pltpu.VMEM((ng - 1, 4, bands), jnp.float32),
            dma((nch,)), dma, dma,
            dma((nch, far)), dma((nch, far)), dma((nch,)), dma((nch,)),
            dma((nch, far)), dma((nch, far)), dma((2, nq)), dma((2, nq)),
            dma((ng - 1,)), dma((ng - 1,)),
        ],
        compiler_params=pltpu.CompilerParams(
            collective_id=0, has_side_effects=True, vmem_limit_bytes=56 * 1024 * 1024),
        name="ritz_residual",
    )(psi.transpose(1, 0, 2), ritz_matrix, potential)
    return rot.transpose(1, 0, 2), search.transpose(1, 0, 2)


def solution(mesh):
    nb, ng = mesh.shape["band"], mesh.shape["grid"]
    return jax.shard_map(
        functools.partial(shards, nb, ng),
        mesh=mesh,
        in_specs=(P("band", "grid", None), P("band", None), P("grid", None)),
        out_specs=(P("band", "grid", None), P("band", "grid", None)),
        check_vma=False,
    )
```

```python
import functools

import jax
import jax.numpy as jnp
from jax import lax
from jax.experimental import pallas as pl
from jax.experimental.pallas import tpu as pltpu
from jax.sharding import PartitionSpec as P

NZ = 64
CW = 128
EPS = 1e-06
MESH = pl.DeviceIdType.MESH


def fused(nb, ng, psi, ritz, pot, rot_out, search_out,
          raw, ritz_f, ritz_s, buf, acc, stencil, rot, halo, resid, part, sums, gat,
          own_sem, ritz_sem, out_sem, far_send, far_recv, near_send, near_recv,
          fwd_send, fwd_recv, halo_send, halo_recv, red_send, red_recv):
    planes, bands, cells = rot.shape
    nq = cells // CW
    chunks = [(p, q) for q in range(nq) for p in range(planes)]
    nchip = nb // 2
    b = lax.axis_index("band")
    g = lax.axis_index("grid")
    chip, core = b // 2, b % 2
    sib = chip * 2 + (1 - core)
    up, down = lax.rem(g + 1, ng), lax.rem(g + ng - 1, ng)

    def far_of(o):
        return lax.rem(chip + o, nchip)

    barrier = pltpu.get_barrier_semaphore()
    for o in range(1, nchip):
        pl.semaphore_signal(barrier, inc=1, device_id={"band": far_of(o) * 2 + core}, device_id_type=MESH)
    pl.semaphore_signal(barrier, inc=1, device_id={"band": sib}, device_id_type=MESH)
    for o in range(1, ng):
        pl.semaphore_signal(barrier, inc=1, device_id={"grid": lax.rem(g + o, ng)}, device_id_type=MESH)

    raws = []
    for q in range(nq):
        raws.append(pltpu.make_async_copy(psi.at[:, :, pl.ds(q * CW, CW)], raw.at[q], own_sem.at[q]))
        raws[q].start()
    ritz_copy = pltpu.make_async_copy(ritz, ritz_f, ritz_sem)
    ritz_copy.start()
    for q in range(nq):
        raws[q].wait()
        for p in range(planes):
            buf[q, b, :, pl.ds(p * CW, CW)] = raw[q, :, p, :]

    pl.semaphore_wait(barrier, nchip - 1 + 1 + ng - 1)

    far = {}
    near = []
    for c, (p, q) in enumerate(chunks):
        mine = buf.at[q, b, :, pl.ds(p * CW, CW)]
        for o in range(1, nchip):
            copy = pltpu.make_async_remote_copy(
                src_ref=mine, dst_ref=mine,
                send_sem=far_send.at[c, o - 1], recv_sem=far_recv.at[c, o - 1],
                device_id={"band": far_of(o) * 2 + core}, device_id_type=MESH)
            copy.start()
            far[c, o] = copy
    for q in range(nq):
        copy = pltpu.make_async_remote_copy(
            src_ref=buf.at[q, b], dst_ref=buf.at[q, b],
            send_sem=near_send.at[q], recv_sem=near_recv.at[q],
            device_id={"band": sib}, device_id_type=MESH)
        copy.start()
        near.append(copy)

    ritz_copy.wait()
    rows = min(bands, 32)

    def split(i, carry):
        at = pl.ds(pl.multiple_of(i * rows, rows), rows)
        whole = ritz_f[at, :]
        hi = whole.astype(jnp.bfloat16)
        rest = whole - hi.astype(jnp.float32)
        mid = rest.astype(jnp.bfloat16)
        ritz_s[0, at, :] = hi
        ritz_s[1, at, :] = mid
        ritz_s[2, at, :] = (rest - mid.astype(jnp.float32)).astype(jnp.bfloat16)
        return carry

    lax.fori_loop(0, bands // rows, split, 0)

    def product(block, first, width):
        at = pl.ds(pl.multiple_of(first * bands, width), width)
        total = jnp.dot(ritz_s[0, :, at], block, preferred_element_type=jnp.float32)
        total += jnp.dot(ritz_s[1, :, at], block, preferred_element_type=jnp.float32)
        total += jnp.dot(ritz_s[2, :, at], block, preferred_element_type=jnp.float32)
        return total

    ny = cells // NZ

    def build(i, carry):
        at = pl.ds(pl.multiple_of(i * 64, 64), 64)
        row = lax.broadcasted_iota(jnp.int32, (64, cells), 0) + i * 64
        col = lax.broadcasted_iota(jnp.int32, (64, cells), 1)
        dy = lax.rem(row // NZ - col // NZ + ny, ny)
        dz = lax.rem(lax.rem(row, NZ) - lax.rem(col, NZ) + NZ, NZ)

        def one(test):
            return jnp.where(test, 1.0, 0.0)

        mat = jnp.where(dz == 0, one(dy == 1) + one(dy == ny - 1), 0.0)
        mat += jnp.where(dy == 0, one(dz == 1) + one(dz == NZ - 1), 0.0)
        mat -= 6.0 * one(row == col)
        stencil[at, :] = mat.astype(jnp.bfloat16)
        return carry

    pair = 2 * bands
    wide = pair % 128 == 0 and bands % 128 != 0
    halos = []
    for q in range(nq):
        near[q].wait_recv()
        acc[...] = product(buf[q, pl.ds(chip * 2, 2)].reshape(pair, planes * CW), chip * 2, pair)
        if q == 0:
            lax.fori_loop(0, cells // 64, build, 0)
        for p in range(planes):
            c = q * planes + p
            lanes = pl.ds(p * CW, CW)
            forwards = []
            for o in range(1, nchip):
                src = far_of(nchip - o) * 2 + core
                far[c, o].wait_recv()
                copy = pltpu.make_async_remote_copy(
                    src_ref=buf.at[q, src, :, lanes], dst_ref=buf.at[q, src, :, lanes],
                    send_sem=fwd_send.at[c, o - 1], recv_sem=fwd_recv.at[c, o - 1],
                    device_id={"band": sib}, device_id_type=MESH)
                copy.start()
                forwards.append(copy)
            for o in range(1, nchip):
                there = far_of(nchip - o) * 2
                if wide:
                    forwards[o - 1].wait_recv()
                    acc[:, lanes] += product(buf[q, pl.ds(there, 2), :, lanes].reshape(pair, CW), there, pair)
                else:
                    acc[:, lanes] += product(buf[q, there + core, :, lanes], there + core, bands)
                    forwards[o - 1].wait_recv()
                    acc[:, lanes] += product(buf[q, there + 1 - core, :, lanes], there + 1 - core, bands)
            at = pl.ds(q * CW, CW)
            rot[p, :, at] = acc[:, lanes].astype(jnp.bfloat16)
            for side, edge, to in ((0, planes - 1, up), (1, 0, down)):
                if p == edge:
                    copy = pltpu.make_async_remote_copy(
                        src_ref=rot.at[p, :, at], dst_ref=halo.at[side, q],
                        send_sem=halo_send.at[side, q], recv_sem=halo_recv.at[side, q],
                        device_id={"grid": to}, device_id_type=MESH)
                    copy.start()
                    halos.append((side, q, copy))
            for copy in forwards:
                copy.wait_send()

    rot_copy = pltpu.make_async_copy(rot, rot_out, out_sem)
    rot_copy.start()

    vr = min(bands, 64)
    for p in range(planes):
        def local(i, carry):
            at = pl.ds(pl.multiple_of(i * vr, vr), vr)
            center = rot[p, at, :]
            lap = jnp.dot(center, stencil[...], preferred_element_type=jnp.float32)
            for other in (p - 1, p + 1):
                if 0 <= other < planes:
                    lap += rot[other, at, :].astype(jnp.float32)
            resid[p, at, :] = -0.5 * lap + pot[pl.ds(p, 1), :] * center.astype(jnp.float32)
            return carry

        lax.fori_loop(0, bands // vr, local, 0)

    part[...] = jnp.zeros_like(part)

    def gather_sums(p, q):
        def body(i, carry):
            at = pl.ds(pl.multiple_of(i * vr, vr), vr)
            lanes = pl.ds(q * CW, CW)
            center = rot[p, at, lanes].astype(jnp.float32)
            value = resid[p, at, lanes]
            if p == 0:
                value -= 0.5 * halo[0, q, at, :].astype(jnp.float32)
            if p == planes - 1:
                value -= 0.5 * halo[1, q, at, :].astype(jnp.float32)
            resid[p, at, lanes] = value
            part[0, at, :] += center * value
            part[1, at, :] += center * center
            part[2, at, :] += value * value
            return carry

        lax.fori_loop(0, bands // vr, body, 0)

    for q in range(nq):
        for side, hq, copy in halos:
            if hq == q:
                copy.wait_recv()
        for p in range(planes):
            gather_sums(p, q)

    for k in range(3):
        sums[pl.ds(k, 1), :] = jnp.sum(part[k].T, axis=0, keepdims=True)
    sums[pl.ds(3, 1), :] = jnp.zeros((1, bands), jnp.float32)

    reds = []
    for o in range(1, ng):
        copy = pltpu.make_async_remote_copy(
            src_ref=sums, dst_ref=gat.at[o - 1],
            send_sem=red_send.at[o - 1], recv_sem=red_recv.at[o - 1],
            device_id={"grid": lax.rem(g + o, ng)}, device_id_type=MESH)
        copy.start()
        reds.append(copy)
    total = sums[...]
    for o in range(1, ng):
        reds[o - 1].wait_recv()
        total = total + gat[o - 1]

    count = float(planes * cells * ng)
    m_cross = total[0:1] / count
    m_plain = total[1:2] / count
    ratio = m_cross / (m_plain + EPS)
    m_dir = total[2:3] / count - 2.0 * ratio * m_cross + ratio * ratio * m_plain
    scale = lax.rsqrt(m_dir + EPS)
    part[0] = jnp.broadcast_to(ratio, (CW, bands)).T
    part[1] = jnp.broadcast_to(scale, (CW, bands)).T

    for p in range(planes):
        def last(i, carry):
            at = pl.ds(pl.multiple_of(i * vr, vr), vr)
            for q in range(nq):
                lanes = pl.ds(q * CW, CW)
                direction = resid[p, at, lanes] - part[0, at, :] * rot[p, at, lanes].astype(jnp.float32)
                search_out[p, at, lanes] = (direction * part[1, at, :]).astype(jnp.bfloat16)
            return carry

        lax.fori_loop(0, bands // vr, last, 0)

    rot_copy.wait()
    for copy in far.values():
        copy.wait_send()
    for copy in near:
        copy.wait_send()
    for _, _, copy in halos:
        copy.wait_send()
    for copy in reds:
        copy.wait_send()


def weave(rot, search, rot_out, search_out):
    for p in range(rot.shape[0]):
        rot_out[:, p, :] = rot[p]
        search_out[:, p, :] = search[p]


def shards(nb, ng, psi, ritz_matrix, potential):
    bands, planes, cells = psi.shape
    total = ritz_matrix.shape[1]
    nq = cells // CW
    nch = nq * planes
    far = max(nb // 2 - 1, 1)
    dma = pltpu.SemaphoreType.DMA
    rot, search = pl.pallas_call(
        functools.partial(fused, nb, ng),
        out_shape=[jax.ShapeDtypeStruct((planes, bands, cells), jnp.bfloat16)] * 2,
        in_specs=[pl.BlockSpec(memory_space=pl.ANY), pl.BlockSpec(memory_space=pl.ANY),
                  pl.BlockSpec(memory_space=pltpu.VMEM)],
        out_specs=[pl.BlockSpec(memory_space=pl.ANY), pl.BlockSpec(memory_space=pltpu.VMEM)],
        scratch_shapes=[
            pltpu.VMEM((nq, bands, planes, CW), jnp.bfloat16),
            pltpu.VMEM((bands, total), jnp.float32),
            pltpu.VMEM((3, bands, total), jnp.bfloat16),
            pltpu.VMEM((nq, nb, bands, planes * CW), jnp.bfloat16),
            pltpu.VMEM((bands, planes * CW), jnp.float32),
            pltpu.VMEM((cells, cells), jnp.bfloat16),
            pltpu.VMEM((planes, bands, cells), jnp.bfloat16),
            pltpu.VMEM((2, nq, bands, CW), jnp.bfloat16),
            pltpu.VMEM((planes, bands, cells), jnp.float32),
            pltpu.VMEM((3, bands, CW), jnp.float32),
            pltpu.VMEM((4, bands), jnp.float32),
            pltpu.VMEM((ng - 1, 4, bands), jnp.float32),
            dma((nq,)), dma, dma,
            dma((nch, far)), dma((nch, far)), dma((nq,)), dma((nq,)),
            dma((nch, far)), dma((nch, far)), dma((2, nq)), dma((2, nq)),
            dma((ng - 1,)), dma((ng - 1,)),
        ],
        compiler_params=pltpu.CompilerParams(
            collective_id=0, has_side_effects=True, vmem_limit_bytes=56 * 1024 * 1024),
        name="ritz_residual",
    )(psi, ritz_matrix, potential)
    step = min(bands, 128)
    inner = pl.BlockSpec((planes, step, cells), lambda i: (0, i, 0))
    outer = pl.BlockSpec((step, planes, cells), lambda i: (i, 0, 0))
    return pl.pallas_call(
        weave,
        grid=(bands // step,),
        out_shape=[jax.ShapeDtypeStruct((bands, planes, cells), jnp.bfloat16)] * 2,
        in_specs=[inner] * 2,
        out_specs=[outer] * 2,
        name="weave",
    )(rot, search)


def solution(mesh):
    nb, ng = mesh.shape["band"], mesh.shape["grid"]
    return jax.shard_map(
        functools.partial(shards, nb, ng),
        mesh=mesh,
        in_specs=(P("band", "grid", None), P("band", None), P("grid", None)),
        out_specs=(P("band", "grid", None), P("band", "grid", None)),
        check_vma=False,
    )
```
